128 devices in a mesh: dp: 8 (over z_hi, y), seq: 16 (over z_lo, x, core).
Axes of the slice: x: 4, y: 4, z: 4 (z_hi: 2, z_lo: 2; z = z_hi * 2 + z_lo), core: 2. Of those that a mesh axis runs over, the one named last changes fastest.
Arguments:
- queries: bfloat16 [65536, 128], P(('dp', 'seq')), parts along dimension 0, may hold values from -384 to 384
- users_of: int32 [65536], P(('dp', 'seq')), parts along dimension 0, may hold values from 0 to 3, as said below
- keys: bfloat16 [32, 16384, 128], P('dp', 'seq'), parts along dimension 0, may hold values from -12 to 12
- values: bfloat16 [32, 16384, 128], P('dp', 'seq'), parts along dimension 0, may hold values from -24 to 24
- lengths: int32 [32], P('dp'), parts along dimension 0, may hold values from 2 to 16384
Outputs:
- pooled: bfloat16 [65536, 128], P(('dp', 'seq')), parts along dimension 0
The draws below stay inside these ranges and needn't reach their ends.
There are 8 independent parts, one for each index of `dp`. The reference program is written for one: setup_inputs(seed, part) draws one part's arguments, and reference() takes and returns one part's arrays. A program takes and returns all parts, laid end to end along the dimension named above; each array names one. Nothing has to cross between parts.
Inputs may be any that keep to these rules, and one draw needn't show every extreme that they name: `users_of`: each candidate names one user of its group.
All inputs are finite; a program needn't handle non-finite values.
Results may differ from the reference program's by a relative error of at most 0.0065.
Values may be sent and summed in bfloat16 or wider, within the bound.
No kernel may reach another device: no remote copies, remote signals or barrier semaphores. Data moves between devices by JAX's collectives and lax.ppermute only.
A program may use at most 192 MiB of HBM per device.

```python
import math
import jax
import jax.numpy as jnp
from jax import lax

D = 128
USERS = 4
CAND_DEV = 512
HIST = 16384
CANDS = 8192


def owner_draw(key):
    return jax.random.randint(jax.random.fold_in(key, 11), (CANDS,), 0, USERS, dtype=jnp.int32)


def key_field(key):
    field_rows = jax.random.normal(jax.random.fold_in(key, 23), (USERS, HIST, D), jnp.float32)
    field_rows = jnp.clip(field_rows, -6.0, 6.0)
    return field_rows


def draw_users_of(key, part):
    return owner_draw(key)


def draw_keys(key, part):
    return key_field(key).astype(jnp.bfloat16)


def draw_queries(key, part):
    drawn_rows = jnp.clip(2.0 * jax.random.normal(jax.random.fold_in(key, 31), (CANDS, D), jnp.float32), -12.0, 12.0)
    return drawn_rows.astype(jnp.bfloat16)


def with_ends(array, own_key, smallest, high):
    spot = [jax.random.randint(jax.random.fold_in(own_key, axis), (), 0, length) for axis, length in enumerate(array.shape)]
    longest = array.shape.index(max(array.shape))
    beside = spot[:longest] + [(spot[longest] + 1) % array.shape[longest]] + spot[longest + 1:]
    return array.at[tuple(spot)].set(smallest).at[tuple(beside)].set(high)


def level_of(stream_key, shape, split, smallest, high):
    def one(position, parts):
        heights = jax.random.uniform(jax.random.fold_in(jax.random.fold_in(stream_key, 6), position), (parts,), jnp.float32, smallest / len(split), high / len(split))
        return jnp.repeat(jnp.exp(heights), shape[position] // parts).reshape((-1,) + (1,) * (len(shape) - position - 1))

    factor_of = one(*split[0])
    for cut in split[1:]:
        factor_of = factor_of * one(*cut)
    return factor_of


def normal_values(rng, dims, scale, most, cuts=(), held_as=jnp.bfloat16):
    values = jax.random.normal(rng, dims, jnp.float32) * scale
    if len(cuts) > 0:
        values = level_of(rng, dims, cuts, -0.22, 0.18) * values
    return jnp.clip(values, min=-most, max=most).astype(held_as)


def setup_inputs(seed: int = 0, part: int = 0) -> dict:
    seeds = jax.random.split(jax.random.key(seed), 6)
    part_splits = jax.random.split(jax.random.fold_in(seeds[5], part), 6)
    queries = draw_queries(jax.random.fold_in(jax.random.fold_in(seeds[5], part), 71), part)
    users_of = draw_users_of(jax.random.fold_in(jax.random.fold_in(seeds[5], part), 71), part)
    keys = draw_keys(jax.random.fold_in(jax.random.fold_in(seeds[5], part), 71), part)
    values = normal_values(part_splits[3], (USERS, HIST, D), 4.0, 24.0, ((1, 16),))
    lengths = with_ends(jax.random.randint(part_splits[4], (USERS,), 2, HIST + 1), jax.random.fold_in(part_splits[4], 1), 2, HIST).astype(jnp.int32)
    return dict(queries=queries, users_of=users_of, keys=keys, values=values, lengths=lengths)


def reference(queries, users_of, keys, values, lengths):
    score_scale = 1.0 / math.sqrt(D)
    positions = jnp.arange(HIST, dtype=jnp.int32)

    def one_block(bundle):
        query_rows, owner_ids = bundle
        result = jnp.zeros((query_rows.shape[0], D), jnp.float32)
        for member in range(USERS):
            scores = jnp.dot(query_rows, keys[member].T, preferred_element_type=jnp.float32) * score_scale
            usable = (owner_ids[:, None] == member) & (positions[None, :] < lengths[member])
            scores = jnp.where(usable, scores, jnp.float32(-1e+30))
            row_max = lax.optimization_barrier(jnp.max(scores, axis=1, keepdims=True))
            weights = jnp.where(usable, jnp.exp(scores - row_max), jnp.float32(0.0))
            totals = lax.optimization_barrier(jnp.sum(weights, axis=1, keepdims=True))
            sums = jnp.dot(weights.astype(jnp.bfloat16), values[member], preferred_element_type=jnp.float32)
            mine = (owner_ids == member)[:, None]
            safe_totals = jnp.where(mine, totals, jnp.float32(1.0))
            result = jnp.where(mine, sums / safe_totals, result)
        return result.astype(jnp.bfloat16)
    blocks = CANDS // CAND_DEV
    query_blocks = queries.reshape(blocks, CAND_DEV, D)
    owner_blocks = users_of.reshape(blocks, CAND_DEV)
    return lax.map(one_block, (query_blocks, owner_blocks)).reshape(CANDS, D)
```

```python
import functools
import math

import jax
import jax.numpy as jnp
from jax import lax
from jax.experimental import pallas as pl
from jax.experimental.pallas import tpu as pltpu
from jax.sharding import PartitionSpec as P


F32 = jnp.float32
BF16 = jnp.bfloat16
I32 = jnp.int32
UNIT = 16
TILE = 256
EMPTY = -1e30
VMEM = pl.BlockSpec(memory_space=pltpu.VMEM)
SMEM = pl.BlockSpec(memory_space=pltpu.SMEM)


def params():
    return pltpu.CompilerParams(vmem_limit_bytes=60 * 1024 * 1024)


def data_rows(count, users):
    return count + (users - 1) * UNIT


def placing(users_row, users):
    count = users_row.shape[1]
    ids = lax.broadcasted_iota(I32, (8, count), 0)
    mine = jnp.where(ids == users_row, 1.0, 0.0).astype(F32)
    before = jnp.where(
        lax.broadcasted_iota(I32, (count, count), 0) < lax.broadcasted_iota(I32, (count, count), 1), 1.0, 0.0
    ).astype(BF16)
    rank = jnp.dot(mine.astype(BF16), before, preferred_element_type=F32)
    units = jnp.floor((jnp.sum(mine, axis=1, keepdims=True) + (UNIT - 1)) * (1.0 / UNIT))
    start = jnp.zeros((1, 1), F32)
    place = jnp.zeros((1, count), F32)
    runs = []
    for user in range(users):
        place += mine[user : user + 1] * (start * UNIT + rank[user : user + 1])
        runs.append(units[user : user + 1])
        start += runs[-1]
    return place.astype(I32), runs, start


def sort_kernel(users, users_ref, q_ref, out_ref):
    count, width = q_ref.shape
    rows = data_rows(count, users)
    place, runs, _ = placing(users_ref[...], users)
    onehot = jnp.where(lax.broadcasted_iota(I32, (rows, count), 0) == place, 1.0, 0.0).astype(BF16)
    out_ref[:rows] = jnp.dot(onehot, q_ref[...], preferred_element_type=F32).astype(BF16)
    lane = lax.broadcasted_iota(I32, (UNIT, width), 1)
    head = jnp.zeros((UNIT, width), F32)
    for user in range(users):
        head += jnp.where(lane == user, runs[user], 0.0)
    out_ref[rows:] = head.astype(BF16)


def prepare_kernel(meta_ref, lengths_ref, k_own, v_own, k_other, v_other, k_out, v_out):
    users, chunk, width = k_own.shape
    rank = meta_ref[0]
    core = lax.rem(rank, 2)
    positions = lax.broadcasted_iota(I32, (chunk, width), 0)
    for user in range(users):
        first = jnp.where(core == 0, k_own[user, :UNIT].astype(F32), k_other[user, :UNIT].astype(F32))[:1]
        for k_ref, v_ref, slot, block in (
            (k_own, v_own, core, rank),
            (k_other, v_other, 1 - core, rank + 1 - 2 * core),
        ):
            usable = positions < lengths_ref[user] - block * chunk
            at = pl.ds(pl.multiple_of(slot * chunk, chunk), chunk)
            k_out[user, at, :] = jnp.where(usable, k_ref[user].astype(F32), first).astype(BF16)
            v_out[user, at, :width] = jnp.where(usable, v_ref[user].astype(F32), 0.0).astype(BF16)
            v_out[user, at, width:] = jnp.where(usable, 1.0, 0.0).astype(BF16)


def attend_kernel(users, blocks, meta_ref, lengths_ref, k_ref, v_ref, *refs):
    q_refs, out_refs = refs[:blocks], refs[blocks : 2 * blocks]
    sorted_q, pooled, stats, turned, heads, counts, sem = refs[2 * blocks :]
    width = k_ref.shape[2]
    held = k_ref.shape[1]
    rows = q_refs[0].shape[0] - UNIT
    score_scale = 1.0 / math.sqrt(width)
    for block in range(blocks):
        heads[block : block + 1] = q_refs[block][rows:].astype(F32)[:1].astype(I32)
    copy = pltpu.make_async_copy(heads, counts, sem)
    copy.start()
    copy.wait()

    run = [[counts[block, user] for user in range(users)] for block in range(blocks)]
    source = [[sum(run[block][:user], jnp.int32(0)) for user in range(users)] for block in range(blocks)]
    at = [[None] * users for _ in range(blocks)]
    begin, total = [], jnp.int32(0)
    for user in range(users):
        begin.append(total)
        for block in range(blocks):
            at[block][user] = total

            def take(i, carry, block=block, user=user, total=total):
                down = pl.multiple_of((source[block][user] + 2 * i) * UNIT, UNIT)
                up = pl.multiple_of((total + 2 * i) * UNIT, UNIT)
                sorted_q[pl.ds(up, 2 * UNIT), :] = q_refs[block][pl.ds(down, 2 * UNIT), :]
                return carry

            lax.fori_loop(0, (run[block][user] + 1) // 2, take, 0)
            total = total + run[block][user]
    begin.append(total)

    lane = lax.broadcasted_iota(I32, (TILE, width), 1)
    part = lax.rem(lane, 16) // 5

    def put(where, mean, level):
        high = level.astype(BF16).astype(F32)
        rest = level - high
        middle = rest.astype(BF16).astype(F32)
        pooled[where, :] = mean.astype(BF16)
        stats[where, :] = jnp.where(part == 0, high, jnp.where(part == 1, middle, rest - middle))

    def spot(user, i):
        return pl.ds(pl.multiple_of(begin[user] * UNIT + i * TILE, UNIT), TILE)

    def step(user, size, i, carry):
        where = spot(user, i)
        scores = lax.dot_general(
            sorted_q[where, :], k_ref[user, :size], (((1,), (1,)), ((), ())), preferred_element_type=F32
        )
        largest = jnp.max(scores, axis=1, keepdims=True)
        factor = score_scale * math.log2(math.e)
        weights = jnp.exp2(scores * factor - largest * factor).astype(BF16)
        sums = jnp.dot(weights, v_ref[user, :size], preferred_element_type=F32)
        totals = sums[:, width:]
        put(where, sums[:, :width] / totals, largest * score_scale + jnp.log(totals))
        return carry

    def skip(user, i, carry):
        put(spot(user, i), jnp.zeros((TILE, width), F32), jnp.full((TILE, width), EMPTY, F32))
        return carry

    for user in range(users):
        usable = lengths_ref[user] - (meta_ref[0] // 2) * held
        tiles = ((begin[user + 1] - begin[user]) * UNIT + TILE - 1) // TILE
        few = 256

        @pl.when(usable > few)
        def _(user=user, tiles=tiles):
            lax.fori_loop(0, tiles, functools.partial(step, user, held), 0)

        @pl.when((usable > 0) & (usable <= few))
        def _(user=user, tiles=tiles):
            lax.fori_loop(0, tiles, functools.partial(step, user, few), 0)

        @pl.when(usable <= 0)
        def _(user=user, tiles=tiles):
            lax.fori_loop(0, tiles, functools.partial(skip, user), 0)

    turned[...] = jnp.zeros_like(turned)
    lane = lax.broadcasted_iota(I32, (UNIT, width), 1)
    code = jnp.where(lax.rem(lane, 16) == 15, -1, (lane // 16) * 8 + lax.rem(lax.rem(lane, 16), 5))
    for block in range(blocks):
        for user in range(users):

            def give(i, carry, block=block, user=user):
                down = pl.multiple_of((at[block][user] + i) * UNIT, UNIT)
                unit = source[block][user] + i
                out_refs[block][pl.ds(pl.multiple_of(unit * UNIT, UNIT), UNIT), :] = pooled[pl.ds(down, UNIT), :]
                spread = pl.ds(pl.multiple_of(lax.rem(unit, 8) * UNIT, UNIT), UNIT)
                turned[spread, :] = jnp.where(
                    code == block * 8 + unit // 8, stats[pl.ds(down, UNIT), :], turned[spread, :]
                )
                return carry

            lax.fori_loop(0, run[block][user], give, 0)
    levels = jnp.transpose(turned[...]).astype(BF16)
    for block in range(blocks):
        out_refs[block][rows:] = levels[block * 16 : block * 16 + 16]


def merge_kernel(users, users_ref, *refs):
    part_refs, out_ref = refs[:-1], refs[-1]
    rows = part_refs[0].shape[0] - UNIT
    width = part_refs[0].shape[1]
    count = users_ref.shape[1]
    groups = 5
    levels = []
    for ref in part_refs:
        pieces = ref[rows:].astype(F32)
        levels.append(pieces[0:5] + pieces[5:10] + pieces[10:15])
    largest = functools.reduce(jnp.maximum, levels)
    shares = [jnp.exp(level - largest) for level in levels]
    whole = sum(shares)
    gap = jnp.zeros((3, width), F32)
    stacked = jnp.concatenate([x for share in shares for x in (share / whole, gap)], axis=0)
    stacked = jnp.concatenate([stacked, jnp.zeros((128 - stacked.shape[0], width), F32)], axis=0)
    columns = jnp.transpose(stacked)
    place, _, used = placing(users_ref[...], users)
    merged = []
    for group in range(groups):
        size = min(128, rows - group * 128)
        total = jnp.zeros((size, width), F32)
        for i, ref in enumerate(part_refs):
            share = columns[:size, i * 8 + group : i * 8 + group + 1]
            total += share * ref[group * 128 : group * 128 + size].astype(F32)
        inside = lax.broadcasted_iota(I32, (size, width), 0) + group * 128 < used.astype(I32) * UNIT
        merged.append(jnp.where(inside, total, 0.0).astype(BF16))
    merged = jnp.concatenate(merged, axis=0)
    onehot = jnp.where(lax.broadcasted_iota(I32, (rows, count), 0) == place, 1.0, 0.0).astype(BF16)
    out_ref[...] = lax.dot_general(
        onehot, merged, (((0,), (0,)), ((), ())), preferred_element_type=F32
    ).astype(BF16)


def local(layout, queries, users_of, keys, values, lengths):
    count, width = queries.shape
    users, chunk, _ = keys.shape
    rows = data_rows(count, users)
    zs, xs = layout

    def shift(dz, dx, dc):
        def place(z, x, c):
            return (z * xs + x) * 2 + c

        return [
            (place(z, x, c), place((z + dz) % zs, (x + dx) % xs, c ^ dc))
            for z in range(zs)
            for x in range(xs)
            for c in range(2)
        ]

    others = [(dz, dx) for dx in range(xs) for dz in range(zs) if (dz, dx) != (0, 0)]
    blocks = len(others) + 1
    meta = lax.axis_index("seq").astype(I32).reshape(1)
    users_row = users_of.reshape(1, count)
    message = jax.ShapeDtypeStruct((rows + UNIT, width), BF16)

    sent = pl.pallas_call(
        functools.partial(sort_kernel, users),
        out_shape=message,
        in_specs=[VMEM, VMEM],
        out_specs=VMEM,
        compiler_params=params(),
    )(users_row, queries)
    k_other = lax.ppermute(keys, "seq", shift(0, 0, 1))
    v_other = lax.ppermute(values, "seq", shift(0, 0, 1))
    arrived = [lax.ppermute(sent, "seq", shift(dz, dx, 0)) for dz, dx in others]

    k_held, v_held = pl.pallas_call(
        prepare_kernel,
        out_shape=(
            jax.ShapeDtypeStruct((users, 2 * chunk, width), BF16),
            jax.ShapeDtypeStruct((users, 2 * chunk, 2 * width), BF16),
        ),
        in_specs=[SMEM, SMEM, VMEM, VMEM, VMEM, VMEM],
        out_specs=(VMEM, VMEM),
        compiler_params=params(),
        cost_estimate=pl.CostEstimate(flops=10**8, bytes_accessed=10**7, transcendentals=0),
    )(meta, lengths, keys, values, k_other, v_other)

    most = blocks * rows + TILE + 2 * UNIT
    parts = pl.pallas_call(
        functools.partial(attend_kernel, users, blocks),
        out_shape=[message] * blocks,
        in_specs=[SMEM, SMEM] + [VMEM] * (2 + blocks),
        out_specs=[VMEM] * blocks,
        scratch_shapes=[
            pltpu.VMEM((most, width), BF16),
            pltpu.VMEM((most, width), BF16),
            pltpu.VMEM((most, width), F32),
            pltpu.VMEM((128, width), F32),
            pltpu.VMEM((blocks, width), I32),
            pltpu.SMEM((blocks, width), I32),
            pltpu.SemaphoreType.DMA,
        ],
        compiler_params=params(),
        cost_estimate=pl.CostEstimate(flops=10**10, bytes_accessed=10**7, transcendentals=0),
    )(meta, lengths, k_held, v_held, sent, *arrived)
    back = [lax.ppermute(part, "seq", shift(-dz, -dx, 0)) for part, (dz, dx) in zip(parts[1:], others)]

    return pl.pallas_call(
        functools.partial(merge_kernel, users),
        out_shape=jax.ShapeDtypeStruct((count, width), BF16),
        in_specs=[VMEM] * (1 + blocks),
        out_specs=VMEM,
        compiler_params=params(),
    )(users_row, parts[0], *back)


def solution(mesh):
    seq = mesh.shape["seq"]
    layout = (2, seq // 4)
    return jax.shard_map(
        functools.partial(local, layout),
        mesh=mesh,
        in_specs=(
            P(("dp", "seq"), None),
            P(("dp", "seq")),
            P("dp", "seq", None),
            P("dp", "seq", None),
            P("dp"),
        ),
        out_specs=P(("dp", "seq"), None),
        check_vma=False,
    )
```

```python
import functools
import math

import jax
import jax.numpy as jnp
from jax import lax
from jax.experimental import pallas as pl
from jax.experimental.pallas import tpu as pltpu
from jax.sharding import PartitionSpec as P


F32 = jnp.float32
BF16 = jnp.bfloat16
I32 = jnp.int32
UNIT = 16
TILE = 256
STRIP = 256
EMPTY = -1e30
VMEM = pl.BlockSpec(memory_space=pltpu.VMEM)
SMEM = pl.BlockSpec(memory_space=pltpu.SMEM)


def params():
    return pltpu.CompilerParams(vmem_limit_bytes=60 * 1024 * 1024)


def data_rows(count, users):
    return count + (users - 1) * UNIT


def placing(users_row, users):
    count = users_row.shape[1]
    ids = lax.broadcasted_iota(I32, (8, count), 0)
    mine = jnp.where(ids == users_row, 1.0, 0.0).astype(F32)
    before = jnp.where(
        lax.broadcasted_iota(I32, (count, count), 0) < lax.broadcasted_iota(I32, (count, count), 1), 1.0, 0.0
    ).astype(BF16)
    rank = jnp.dot(mine.astype(BF16), before, preferred_element_type=F32)
    units = jnp.floor((jnp.sum(mine, axis=1, keepdims=True) + (UNIT - 1)) * (1.0 / UNIT))
    start = jnp.zeros((1, 1), F32)
    place = jnp.zeros((1, count), F32)
    runs = []
    for user in range(users):
        place += mine[user : user + 1] * (start * UNIT + rank[user : user + 1])
        runs.append(units[user : user + 1])
        start += runs[-1]
    return place.astype(I32), runs


def sort_kernel(users, users_ref, q_ref, out_ref):
    count, width = q_ref.shape
    rows = data_rows(count, users)
    place, runs = placing(users_ref[...], users)
    onehot = jnp.where(lax.broadcasted_iota(I32, (rows, count), 0) == place, 1.0, 0.0).astype(BF16)
    out_ref[:rows] = jnp.dot(onehot, q_ref[...], preferred_element_type=F32).astype(BF16)
    lane = lax.broadcasted_iota(I32, (UNIT, width), 1)
    head = jnp.zeros((UNIT, width), F32)
    for user in range(users):
        head += jnp.where(lane == user, runs[user], 0.0)
    out_ref[rows:] = head.astype(BF16)


def prepare_kernel(meta_ref, lengths_ref, k_own, v_own, k_other, v_other, k_out, v_out):
    users, chunk, width = k_own.shape
    rank = meta_ref[0]
    core = lax.rem(rank, 2)
    down = lax.broadcasted_iota(I32, (chunk, width), 0)
    along = lax.broadcasted_iota(I32, (width, chunk), 1)
    for user in range(users):
        first = jnp.where(core == 0, k_own[user, :UNIT].astype(F32), k_other[user, :UNIT].astype(F32))[:1]
        for k_ref, v_ref, slot, block in (
            (k_own, v_own, core, rank),
            (k_other, v_other, 1 - core, rank + 1 - 2 * core),
        ):
            usable = lengths_ref[user] - block * chunk
            at = pl.ds(pl.multiple_of(slot * chunk, chunk), chunk)
            k_out[user, at, :] = jnp.where(down < usable, k_ref[user].astype(F32), first).astype(BF16)
            turned = jnp.transpose(v_ref[user].astype(F32))
            v_out[user, :width, at] = jnp.where(along < usable, turned, 0.0).astype(BF16)
            v_out[user, width:, at] = jnp.where(along[:UNIT] < usable, 1.0, 0.0).astype(BF16)


def attend_scratch(blocks, rows, width, users=4, held=2048):
    most = attend_rows(blocks, rows, users)
    return [
        pltpu.VMEM((most, width), BF16),
        pltpu.VMEM((most, width), BF16),
        pltpu.VMEM((most, width), F32),
        pltpu.VMEM((held, TILE), F32),
        pltpu.VMEM((held, TILE), F32),
        pltpu.VMEM((16, width), I32),
        pltpu.SMEM((16, width), I32),
        pltpu.SMEM((2, 64), I32),
        pltpu.SemaphoreType.DMA,
    ]


def attend_rows(blocks, rows, users):
    return blocks * rows + users * (TILE - UNIT) + UNIT


def attend_kernel(users, blocks, meta_ref, lengths_ref, k_ref, v_ref, *refs):
    q_refs, out_refs = refs[:blocks], refs[blocks : 2 * blocks]
    sorted_q, pooled, stats, scores_a, scores_b, table, spots, tiles, sem = refs[2 * blocks :]
    width = k_ref.shape[2]
    held = k_ref.shape[1]
    rows = q_refs[0].shape[0] - UNIT
    score_scale = 1.0 / math.sqrt(width)
    factor = score_scale * math.log2(math.e)
    idle = attend_rows(blocks, rows, users) // UNIT - 1
    per_tile = TILE // UNIT

    heads = jnp.concatenate([ref[rows:].astype(F32)[:1] for ref in q_refs], axis=0)
    sub = lax.broadcasted_iota(I32, (blocks, width), 0)
    lane = lax.broadcasted_iota(I32, (blocks, width), 1)
    unit = lane.astype(F32)
    ahead = jnp.zeros((blocks, width), F32)
    for block in range(blocks):
        ahead += jnp.where(sub > block, heads[block : block + 1], 0.0)
    totals = jnp.sum(heads, axis=0, keepdims=True)
    begin = jnp.zeros((1, 1), F32)
    within = jnp.zeros((blocks, 1), F32)
    spot = unit
    facts = jnp.zeros((blocks, width), F32)
    for user in range(users):
        spot = jnp.where(unit >= within, unit - within + begin + ahead[:, user : user + 1], spot)
        within += heads[:, user : user + 1]
        count = jnp.floor((totals[:, user : user + 1] + (per_tile - 1)) * (1.0 / per_tile))
        facts = jnp.where(lane == user, begin, jnp.where(lane == 8 + user, count, facts))
        begin += count * per_tile
    spot = jnp.where(unit >= within, float(idle), spot)
    table[:blocks] = spot.astype(I32)
    table[blocks:] = facts.astype(I32)
    copy = pltpu.make_async_copy(table, spots, sem)
    copy.start()
    copy.wait()

    def spot_of(block, unit):
        return pl.ds(pl.multiple_of(spots[block, unit] * UNIT, UNIT), UNIT)

    units = rows // UNIT
    for block in range(blocks):
        for unit in range(units):
            sorted_q[spot_of(block, unit), :] = q_refs[block][unit * UNIT : (unit + 1) * UNIT]
    pooled[idle * UNIT :] = jnp.zeros((UNIT, width), BF16)
    stats[idle * UNIT :] = jnp.zeros((UNIT, width), F32)

    def tile_at(row):
        return pl.ds(pl.multiple_of(row, TILE), TILE)

    part = lax.rem(lax.broadcasted_iota(I32, (width, TILE), 0), 16) // 5

    def finish(row, sums, largest):
        total = sums[width : width + 1]
        level = largest * score_scale + jnp.log(total)
        high = level.astype(BF16).astype(F32)
        rest = level - high
        middle = rest.astype(BF16).astype(F32)
        pooled[tile_at(row), :] = jnp.transpose(sums[:width] * (1.0 / total)).astype(BF16)
        stats[tile_at(row), :] = jnp.transpose(
            jnp.where(part == 0, high, jnp.where(part == 1, middle, rest - middle))
        )

    def score(buffer, user, query, best, j):
        scores = lax.dot_general(
            k_ref[user, j * STRIP : (j + 1) * STRIP],
            query,
            (((1,), (1,)), ((), ())),
            preferred_element_type=F32,
        )
        buffer[j * STRIP : (j + 1) * STRIP, :] = scores
        strip = jnp.max(scores.reshape(STRIP // 8, 8, TILE), axis=0)
        return strip if best is None else jnp.maximum(best, strip)

    def weigh(buffer, user, scaled, sums, j):
        weights = jnp.exp2(buffer[j * STRIP : (j + 1) * STRIP, :] * factor - scaled).astype(BF16)
        more = jnp.dot(v_ref[user, :, j * STRIP : (j + 1) * STRIP], weights, preferred_element_type=F32)
        return more if sums is None else sums + more

    def both(ahead, ahead_buffer, now, now_buffer, best):
        user, row = tiles[0, ahead], tiles[1, ahead]
        now_user, now_row = tiles[0, now], tiles[1, now]
        query = sorted_q[tile_at(row), :]
        largest = jnp.max(best, axis=0, keepdims=True)
        scaled = largest * factor
        best, sums = None, None
        for j in range(held // STRIP):
            best = score(ahead_buffer, user, query, best, j)
            sums = weigh(now_buffer, now_user, scaled, sums, j)
        finish(now_row, sums, largest)
        return best

    def few_step(user, i, carry):
        row = spots[8, user] * UNIT + i * TILE
        best = score(scores_a, user, sorted_q[tile_at(row), :], None, 0)
        largest = jnp.max(best, axis=0, keepdims=True)
        finish(row, weigh(scores_a, user, largest * factor, None, 0), largest)
        return carry

    def skip_step(user, i, carry):
        row = spots[8, user] * UNIT + i * TILE
        empty = jnp.full((1, TILE), EMPTY, F32)
        sums = jnp.where(lax.broadcasted_iota(I32, (width + UNIT, TILE), 0) < width, 0.0, 1.0)
        finish(row, sums, empty * (1.0 / score_scale))
        return carry

    full = jnp.int32(0)
    for user in range(users):
        usable = lengths_ref[user] - (meta_ref[0] // 2) * held
        count = spots[8, 8 + user]
        many = usable > STRIP

        def enter(i, carry, user=user, full=full):
            tiles[0, full + i] = jnp.int32(user)
            tiles[1, full + i] = spots[8, user] * UNIT + i * TILE
            return carry

        listed = jnp.where(many, count, 0)
        lax.fori_loop(0, listed, enter, 0)
        full = full + listed
        lax.fori_loop(0, jnp.where((usable > 0) & (usable <= STRIP), count, 0), functools.partial(few_step, user), 0)
        lax.fori_loop(0, jnp.where(usable <= 0, count, 0), functools.partial(skip_step, user), 0)

    @pl.when(full > 0)
    def _():
        query = sorted_q[tile_at(tiles[1, 0]), :]
        best = None
        for j in range(held // STRIP):
            best = score(scores_a, tiles[0, 0], query, best, j)

        def pair(i, best):
            last = full - 1
            second = jnp.minimum(2 * i + 1, last)
            best = both(second, scores_b, 2 * i, scores_a, best)
            return both(jnp.minimum(2 * i + 2, last), scores_a, second, scores_b, best)

        lax.fori_loop(0, (full + 1) // 2, pair, best)

    lane = lax.broadcasted_iota(I32, (UNIT, width), 1)
    code = jnp.where(lax.rem(lane, 16) == 15, -1, (lane // 16) * 8 + lax.rem(lax.rem(lane, 16), 5))
    turned = []
    for place in range(8):
        held_rows = jnp.zeros((UNIT, width), F32)
        for unit in range(place, units, 8):
            for block in range(blocks):
                held_rows = jnp.where(code == block * 8 + unit // 8, stats[spot_of(block, unit), :], held_rows)
        turned.append(held_rows)
    levels = jnp.transpose(jnp.concatenate(turned, axis=0)).astype(BF16)
    for block in range(blocks):
        for unit in range(units):
            out_refs[block][unit * UNIT : (unit + 1) * UNIT] = pooled[spot_of(block, unit), :]
        out_refs[block][rows:] = levels[block * 16 : block * 16 + 16]


def merge_kernel(users, users_ref, *refs):
    part_refs, out_ref = refs[:-1], refs[-1]
    rows = part_refs[0].shape[0] - UNIT
    width = part_refs[0].shape[1]
    count = users_ref.shape[1]
    groups = 5
    levels = []
    for ref in part_refs:
        pieces = ref[rows:].astype(F32)
        levels.append(pieces[0:5] + pieces[5:10] + pieces[10:15])
    largest = functools.reduce(jnp.maximum, levels)
    shares = [jnp.exp(level - largest) for level in levels]
    whole = sum(shares)
    gap = jnp.zeros((3, width), F32)
    stacked = jnp.concatenate([x for share in shares for x in (share / whole, gap)], axis=0)
    stacked = jnp.concatenate([stacked, jnp.zeros((128 - stacked.shape[0], width), F32)], axis=0)
    columns = jnp.transpose(stacked)
    place, _ = placing(users_ref[...], users)
    merged = []
    for group in range(groups):
        size = min(128, rows - group * 128)
        total = jnp.zeros((size, width), F32)
        for i, ref in enumerate(part_refs):
            share = columns[:size, i * 8 + group : i * 8 + group + 1]
            total += share * ref[group * 128 : group * 128 + size].astype(F32)
        merged.append(total.astype(BF16))
    merged = jnp.concatenate(merged, axis=0)
    onehot = jnp.where(lax.broadcasted_iota(I32, (rows, count), 0) == place, 1.0, 0.0).astype(BF16)
    out_ref[...] = lax.dot_general(
        onehot, merged, (((0,), (0,)), ((), ())), preferred_element_type=F32
    ).astype(BF16)


def local(layout, queries, users_of, keys, values, lengths):
    count, width = queries.shape
    users, chunk, _ = keys.shape
    rows = data_rows(count, users)
    zs, xs = layout

    def shift(dz, dx, dc):
        def place(z, x, c):
            return (z * xs + x) * 2 + c

        return [
            (place(z, x, c), place((z + dz) % zs, (x + dx) % xs, c ^ dc))
            for z in range(zs)
            for x in range(xs)
            for c in range(2)
        ]

    others = [(dz, dx) for dx in range(xs) for dz in range(zs) if (dz, dx) != (0, 0)]
    blocks = len(others) + 1
    meta = lax.axis_index("seq").astype(I32).reshape(1)
    users_row = users_of.reshape(1, count)
    message = jax.ShapeDtypeStruct((rows + UNIT, width), BF16)

    sent = pl.pallas_call(
        functools.partial(sort_kernel, users),
        out_shape=message,
        in_specs=[VMEM, VMEM],
        out_specs=VMEM,
        compiler_params=params(),
    )(users_row, queries)
    k_other = lax.ppermute(keys, "seq", shift(0, 0, 1))
    v_other = lax.ppermute(values, "seq", shift(0, 0, 1))
    arrived = [lax.ppermute(sent, "seq", shift(dz, dx, 0)) for dz, dx in others]

    k_held, v_held = pl.pallas_call(
        prepare_kernel,
        out_shape=(
            jax.ShapeDtypeStruct((users, 2 * chunk, width), BF16),
            jax.ShapeDtypeStruct((users, width + UNIT, 2 * chunk), BF16),
        ),
        in_specs=[SMEM, SMEM, VMEM, VMEM, VMEM, VMEM],
        out_specs=(VMEM, VMEM),
        compiler_params=params(),
        cost_estimate=pl.CostEstimate(flops=10**8, bytes_accessed=10**7, transcendentals=0),
    )(meta, lengths, keys, values, k_other, v_other)

    parts = pl.pallas_call(
        functools.partial(attend_kernel, users, blocks),
        out_shape=[message] * blocks,
        in_specs=[SMEM, SMEM] + [VMEM] * (2 + blocks),
        out_specs=[VMEM] * blocks,
        scratch_shapes=attend_scratch(blocks, rows, width, users, 2 * chunk),
        compiler_params=params(),
        cost_estimate=pl.CostEstimate(flops=10**10, bytes_accessed=10**7, transcendentals=0),
    )(meta, lengths, k_held, v_held, sent, *arrived)
    back = [lax.ppermute(part, "seq", shift(-dz, -dx, 0)) for part, (dz, dx) in zip(parts[1:], others)]

    return pl.pallas_call(
        functools.partial(merge_kernel, users),
        out_shape=jax.ShapeDtypeStruct((count, width), BF16),
        in_specs=[VMEM] * (1 + blocks),
        out_specs=VMEM,
        compiler_params=params(),
    )(users_row, parts[0], *back)


def solution(mesh):
    seq = mesh.shape["seq"]
    layout = (2, seq // 4)
    return jax.shard_map(
        functools.partial(local, layout),
        mesh=mesh,
        in_specs=(
            P(("dp", "seq"), None),
            P(("dp", "seq")),
            P("dp", "seq", None),
            P("dp", "seq", None),
            P("dp"),
        ),
        out_specs=P(("dp", "seq"), None),
        check_vma=False,
    )
```

```python
import functools
import math

import jax
import jax.numpy as jnp
from jax import lax
from jax.experimental import pallas as pl
from jax.experimental.pallas import tpu as pltpu
from jax.sharding import PartitionSpec as P


F32 = jnp.float32
BF16 = jnp.bfloat16
I32 = jnp.int32
UNIT = 16
TILE = 256
STRIP = 256
EMPTY = -1e30
VMEM = pl.BlockSpec(memory_space=pltpu.VMEM)
SMEM = pl.BlockSpec(memory_space=pltpu.SMEM)


def params(mebibytes):
    return pltpu.CompilerParams(vmem_limit_bytes=mebibytes * 1024 * 1024)


def data_rows(count, users):
    return count + (users - 1) * UNIT


def placing(users_row, users):
    count = users_row.shape[1]
    ids = lax.broadcasted_iota(I32, (8, count), 0)
    mine = jnp.where(ids == users_row, 1.0, 0.0).astype(F32)
    before = jnp.where(
        lax.broadcasted_iota(I32, (count, count), 0) < lax.broadcasted_iota(I32, (count, count), 1), 1.0, 0.0
    ).astype(BF16)
    rank = jnp.dot(mine.astype(BF16), before, preferred_element_type=F32)
    units = jnp.floor((jnp.sum(mine, axis=1, keepdims=True) + (UNIT - 1)) * (1.0 / UNIT))
    start = jnp.zeros((1, 1), F32)
    place = jnp.zeros((1, count), F32)
    runs = []
    for user in range(users):
        place += mine[user : user + 1] * (start * UNIT + rank[user : user + 1])
        runs.append(units[user : user + 1])
        start += runs[-1]
    return place.astype(I32), runs


def sort_kernel(users, users_ref, q_ref, out_ref):
    count, width = q_ref.shape
    rows = data_rows(count, users)
    place, runs = placing(users_ref[...], users)
    onehot = jnp.where(lax.broadcasted_iota(I32, (rows, count), 0) == place, 1.0, 0.0).astype(BF16)
    out_ref[:rows] = jnp.dot(onehot, q_ref[...], preferred_element_type=F32).astype(BF16)
    lane = lax.broadcasted_iota(I32, (UNIT, width), 1)
    head = jnp.zeros((UNIT, width), F32)
    for user in range(users):
        head += jnp.where(lane == user, runs[user], 0.0)
    out_ref[rows:] = head.astype(BF16)


def prepare_kernel(meta_ref, lengths_ref, k_own, v_own, k_other, v_other, k_out, v_out):
    users, chunk, width = k_own.shape
    rank = meta_ref[0]
    core = lax.rem(rank, 2)
    down = lax.broadcasted_iota(I32, (chunk, width), 0)
    along = lax.broadcasted_iota(I32, (width, chunk), 1)
    for user in range(users):
        first = jnp.where(core == 0, k_own[user, :UNIT].astype(F32), k_other[user, :UNIT].astype(F32))[:1]
        for k_ref, v_ref, slot, block in (
            (k_own, v_own, core, rank),
            (k_other, v_other, 1 - core, rank + 1 - 2 * core),
        ):
            usable = lengths_ref[user] - block * chunk
            at = pl.ds(pl.multiple_of(slot * chunk, chunk), chunk)
            k_out[user, at, :] = jnp.where(down < usable, k_ref[user].astype(F32), first).astype(BF16)
            turned = jnp.transpose(v_ref[user].astype(F32))
            v_out[user, :width, at] = jnp.where(along < usable, turned, 0.0).astype(BF16)
            v_out[user, width:, at] = jnp.where(along[:UNIT] < usable, 1.0, 0.0).astype(BF16)


def attend_scratch(blocks, rows, width, users=4, held=2048):
    most = attend_rows(blocks, rows, users)
    return [
        pltpu.VMEM((most, width), BF16),
        pltpu.VMEM((most, width), BF16),
        pltpu.VMEM((most, width), F32),
        pltpu.VMEM((held, TILE), F32),
        pltpu.VMEM((held, TILE), F32),
        pltpu.VMEM((16, width), I32),
        pltpu.SMEM((16, width), I32),
        pltpu.SMEM((2, 64), I32),
        pltpu.SemaphoreType.DMA,
    ]


def attend_rows(blocks, rows, users):
    return blocks * rows + users * (TILE - UNIT) + UNIT


def attend_kernel(users, blocks, meta_ref, lengths_ref, k_ref, v_ref, *refs):
    q_refs, out_refs = refs[:blocks], refs[blocks : 2 * blocks]
    sorted_q, pooled, stats, scores_a, scores_b, table, spots, tiles, sem = refs[2 * blocks :]
    width = k_ref.shape[2]
    held = k_ref.shape[1]
    rows = q_refs[0].shape[0] - UNIT
    score_scale = 1.0 / math.sqrt(width)
    factor = score_scale * math.log2(math.e)
    idle = attend_rows(blocks, rows, users) // UNIT - 1
    per_tile = TILE // UNIT

    heads = jnp.concatenate(
        [ref[rows:].astype(F32)[:1] for ref in q_refs] + [jnp.zeros((1, width), F32)] * (8 - blocks), axis=0
    )
    sub = lax.broadcasted_iota(I32, (8, width), 0)
    lane = lax.broadcasted_iota(I32, (8, width), 1)
    unit = lane.astype(F32)
    ahead = jnp.zeros((8, width), F32)
    for block in range(blocks):
        ahead += jnp.where(sub > block, heads[block : block + 1], 0.0)
    totals = jnp.sum(heads, axis=0, keepdims=True)
    begin = jnp.zeros((1, 1), F32)
    within = jnp.zeros((8, 1), F32)
    spot = unit
    facts = jnp.zeros((8, width), F32)
    for user in range(users):
        spot = jnp.where(unit >= within, unit - within + begin + ahead[:, user : user + 1], spot)
        within += heads[:, user : user + 1]
        count = jnp.floor((totals[:, user : user + 1] + (per_tile - 1)) * (1.0 / per_tile))
        facts = jnp.where(lane == user, begin, jnp.where(lane == 8 + user, count, facts))
        begin += count * per_tile
    spot = jnp.where(unit >= within, float(idle), spot)
    table[:8] = spot.astype(I32)
    table[8:] = facts.astype(I32)
    copy = pltpu.make_async_copy(table, spots, sem)
    copy.start()
    copy.wait()

    def spot_of(block, unit):
        return pl.ds(pl.multiple_of(spots[block, unit] * UNIT, UNIT), UNIT)

    units = rows // UNIT
    for block in range(blocks):
        for unit in range(units):
            sorted_q[spot_of(block, unit), :] = q_refs[block][unit * UNIT : (unit + 1) * UNIT]
    pooled[idle * UNIT :] = jnp.zeros((UNIT, width), BF16)
    stats[idle * UNIT :] = jnp.zeros((UNIT, width), F32)

    def tile_at(row):
        return pl.ds(pl.multiple_of(row, TILE), TILE)

    part = lax.rem(lax.broadcasted_iota(I32, (width, TILE), 0), 16) // 5

    def finish(row, sums, largest):
        total = sums[width : width + 1]
        level = largest * score_scale + jnp.log(total)
        high = level.astype(BF16).astype(F32)
        rest = level - high
        middle = rest.astype(BF16).astype(F32)
        pooled[tile_at(row), :] = jnp.transpose(sums[:width] * (1.0 / total)).astype(BF16)
        stats[tile_at(row), :] = jnp.transpose(
            jnp.where(part == 0, high, jnp.where(part == 1, middle, rest - middle))
        )

    def score(buffer, user, query, best, j):
        scores = lax.dot_general(
            k_ref[user, j * STRIP : (j + 1) * STRIP],
            query,
            (((1,), (1,)), ((), ())),
            preferred_element_type=F32,
        )
        buffer[j * STRIP : (j + 1) * STRIP, :] = scores
        strip = jnp.max(scores.reshape(STRIP // 8, 8, TILE), axis=0)
        return strip if best is None else jnp.maximum(best, strip)

    def weigh(buffer, user, scaled, sums, j):
        weights = jnp.exp2(buffer[j * STRIP : (j + 1) * STRIP, :] * factor - scaled).astype(BF16)
        more = jnp.dot(v_ref[user, :, j * STRIP : (j + 1) * STRIP], weights, preferred_element_type=F32)
        return more if sums is None else sums + more

    def both(ahead, ahead_buffer, now, now_buffer, best):
        user, row = tiles[0, ahead], tiles[1, ahead]
        now_user, now_row = tiles[0, now], tiles[1, now]
        query = sorted_q[tile_at(row), :]
        largest = jnp.max(best, axis=0, keepdims=True)
        scaled = largest * factor
        best, sums = None, None
        for j in range(held // STRIP):
            best = score(ahead_buffer, user, query, best, j)
            sums = weigh(now_buffer, now_user, scaled, sums, j)
        finish(now_row, sums, largest)
        return best

    def few_step(user, i, carry):
        row = spots[8, user] * UNIT + i * TILE
        best = score(scores_a, user, sorted_q[tile_at(row), :], None, 0)
        largest = jnp.max(best, axis=0, keepdims=True)
        finish(row, weigh(scores_a, user, largest * factor, None, 0), largest)
        return carry

    def skip_step(user, i, carry):
        row = spots[8, user] * UNIT + i * TILE
        empty = jnp.full((1, TILE), EMPTY, F32)
        sums = jnp.where(lax.broadcasted_iota(I32, (width + UNIT, TILE), 0) < width, 0.0, 1.0)
        finish(row, sums, empty * (1.0 / score_scale))
        return carry

    full = jnp.int32(0)
    for user in range(users):
        usable = lengths_ref[user] - (meta_ref[0] // 2) * held
        count = spots[8, 8 + user]
        many = usable > STRIP

        def enter(i, carry, user=user, full=full):
            tiles[0, full + i] = jnp.int32(user)
            tiles[1, full + i] = spots[8, user] * UNIT + i * TILE
            return carry

        listed = jnp.where(many, count, 0)
        lax.fori_loop(0, listed, enter, 0)
        full = full + listed
        lax.fori_loop(0, jnp.where((usable > 0) & (usable <= STRIP), count, 0), functools.partial(few_step, user), 0)
        lax.fori_loop(0, jnp.where(usable <= 0, count, 0), functools.partial(skip_step, user), 0)

    @pl.when(full > 0)
    def _():
        query = sorted_q[tile_at(tiles[1, 0]), :]
        best = None
        for j in range(held // STRIP):
            best = score(scores_a, tiles[0, 0], query, best, j)

        def pair(i, best):
            last = full - 1
            second = jnp.minimum(2 * i + 1, last)
            best = both(second, scores_b, 2 * i, scores_a, best)
            return both(jnp.minimum(2 * i + 2, last), scores_a, second, scores_b, best)

        lax.fori_loop(0, (full + 1) // 2, pair, best)

    lane = lax.broadcasted_iota(I32, (UNIT, width), 1)
    code = jnp.where(lax.rem(lane, 16) == 15, -1, (lane // 16) * 8 + lax.rem(lax.rem(lane, 16), 5))
    turned = []
    for place in range(8):
        held_rows = jnp.zeros((UNIT, width), F32)
        for unit in range(place, units, 8):
            for block in range(blocks):
                held_rows = jnp.where(code == block * 8 + unit // 8, stats[spot_of(block, unit), :], held_rows)
        turned.append(held_rows)
    levels = jnp.transpose(jnp.concatenate(turned, axis=0)).astype(BF16)
    for block in range(blocks):
        for unit in range(units):
            out_refs[block][unit * UNIT : (unit + 1) * UNIT] = pooled[spot_of(block, unit), :]
        out_refs[block][rows:] = levels[block * 16 : block * 16 + 16]


def merge_kernel(users, users_ref, *refs):
    part_refs, out_ref = refs[:-1], refs[-1]
    rows = part_refs[0].shape[0] - UNIT
    width = part_refs[0].shape[1]
    count = users_ref.shape[1]
    groups = 5
    levels = []
    for ref in part_refs:
        pieces = ref[rows:].astype(F32)
        levels.append(pieces[0:5] + pieces[5:10] + pieces[10:15])
    largest = functools.reduce(jnp.maximum, levels)
    shares = [jnp.exp(level - largest) for level in levels]
    whole = sum(shares)
    gap = jnp.zeros((3, width), F32)
    stacked = jnp.concatenate([x for share in shares for x in (share / whole, gap)], axis=0)
    stacked = jnp.concatenate([stacked, jnp.zeros((128 - stacked.shape[0], width), F32)], axis=0)
    columns = jnp.transpose(stacked)
    place, _ = placing(users_ref[...], users)
    merged = []
    for group in range(groups):
        size = min(128, rows - group * 128)
        total = jnp.zeros((size, width), F32)
        for i, ref in enumerate(part_refs):
            share = columns[:size, i * 8 + group : i * 8 + group + 1]
            total += share * ref[group * 128 : group * 128 + size].astype(F32)
        merged.append(total.astype(BF16))
    merged = jnp.concatenate(merged, axis=0)
    onehot = jnp.where(lax.broadcasted_iota(I32, (rows, count), 0) == place, 1.0, 0.0).astype(BF16)
    out_ref[...] = lax.dot_general(
        onehot, merged, (((0,), (0,)), ((), ())), preferred_element_type=F32
    ).astype(BF16)


def local(layout, queries, users_of, keys, values, lengths):
    count, width = queries.shape
    users, chunk, _ = keys.shape
    rows = data_rows(count, users)
    zs, xs = layout

    def shift(dz, dx, dc):
        def place(z, x, c):
            return (z * xs + x) * 2 + c

        return [
            (place(z, x, c), place((z + dz) % zs, (x + dx) % xs, c ^ dc))
            for z in range(zs)
            for x in range(xs)
            for c in range(2)
        ]

    near = [(0, 1), (0, xs - 1), (1, 0), (1, 1)]
    far = [(dz, dx) for dz in range(zs) for dx in range(xs) if (dz, dx) not in near and (dz, dx) != (0, 0)]
    meta = lax.axis_index("seq").astype(I32).reshape(1)
    users_row = users_of.reshape(1, count)
    message = jax.ShapeDtypeStruct((rows + UNIT, width), BF16)

    sent = pl.pallas_call(
        functools.partial(sort_kernel, users),
        out_shape=message,
        in_specs=[VMEM, VMEM],
        out_specs=VMEM,
        compiler_params=params(8),
    )(users_row, queries)
    k_other = lax.ppermute(keys, "seq", shift(0, 0, 1))
    v_other = lax.ppermute(values, "seq", shift(0, 0, 1))
    near_in = [lax.ppermute(sent, "seq", shift(dz, dx, 0)) for dz, dx in near]
    far_in = [lax.ppermute(sent, "seq", shift(dz, dx, 0)) for dz, dx in far]

    k_held, v_held = pl.pallas_call(
        prepare_kernel,
        out_shape=(
            jax.ShapeDtypeStruct((users, 2 * chunk, width), BF16),
            jax.ShapeDtypeStruct((users, width + UNIT, 2 * chunk), BF16),
        ),
        in_specs=[SMEM, SMEM, VMEM, VMEM, VMEM, VMEM],
        out_specs=(VMEM, VMEM),
        compiler_params=params(20),
        cost_estimate=pl.CostEstimate(flops=10**8, bytes_accessed=10**7, transcendentals=0),
    )(meta, lengths, keys, values, k_other, v_other)

    def attend(arrived):
        blocks = len(arrived)
        return pl.pallas_call(
            functools.partial(attend_kernel, users, blocks),
            out_shape=[message] * blocks,
            in_specs=[SMEM, SMEM] + [VMEM] * (2 + blocks),
            out_specs=[VMEM] * blocks,
            scratch_shapes=attend_scratch(blocks, rows, width, users, 2 * chunk),
            compiler_params=params(24),
            cost_estimate=pl.CostEstimate(flops=10**10, bytes_accessed=10**7, transcendentals=0),
        )(meta, lengths, k_held, v_held, *arrived)

    own, *near_out = attend([sent, *near_in])
    near_back = [lax.ppermute(part, "seq", shift(-dz, -dx, 0)) for part, (dz, dx) in zip(near_out, near)]
    far_out = attend(far_in)
    far_back = [lax.ppermute(part, "seq", shift(-dz, -dx, 0)) for part, (dz, dx) in zip(far_out, far)]
    blocks = 1 + len(near) + len(far)

    return pl.pallas_call(
        functools.partial(merge_kernel, users),
        out_shape=jax.ShapeDtypeStruct((count, width), BF16),
        in_specs=[VMEM] * (1 + blocks),
        out_specs=VMEM,
        compiler_params=params(8),
    )(users_row, own, *near_back, *far_back)


def solution(mesh):
    seq = mesh.shape["seq"]
    layout = (2, seq // 4)
    return jax.shard_map(
        functools.partial(local, layout),
        mesh=mesh,
        in_specs=(
            P(("dp", "seq"), None),
            P(("dp", "seq")),
            P("dp", "seq", None),
            P("dp", "seq", None),
            P("dp"),
        ),
        out_specs=P(("dp", "seq"), None),
        check_vma=False,
    )
```

```python
import functools
import math

import jax
import jax.numpy as jnp
from jax import lax
from jax.experimental import pallas as pl
from jax.experimental.pallas import tpu as pltpu
from jax.sharding import PartitionSpec as P


F32 = jnp.float32
BF16 = jnp.bfloat16
I32 = jnp.int32
UNIT = 16
TILE = 256
STRIP = 256
EMPTY = -1e30
VMEM = pl.BlockSpec(memory_space=pltpu.VMEM)
SMEM = pl.BlockSpec(memory_space=pltpu.SMEM)
HBM = pl.BlockSpec(memory_space=pltpu.HBM)


def params(mebibytes):
    return pltpu.CompilerParams(vmem_limit_bytes=mebibytes * 1024 * 1024)


def data_rows(count, users):
    return count + (users - 1) * UNIT


def placing(users_row, users):
    count = users_row.shape[1]
    ids = lax.broadcasted_iota(I32, (8, count), 0)
    mine = jnp.where(ids == users_row, 1.0, 0.0).astype(F32)
    before = jnp.where(
        lax.broadcasted_iota(I32, (count, count), 0) < lax.broadcasted_iota(I32, (count, count), 1), 1.0, 0.0
    ).astype(BF16)
    rank = jnp.dot(mine.astype(BF16), before, preferred_element_type=F32)
    units = jnp.floor((jnp.sum(mine, axis=1, keepdims=True) + (UNIT - 1)) * (1.0 / UNIT))
    start = jnp.zeros((1, 1), F32)
    place = jnp.zeros((1, count), F32)
    runs = []
    for user in range(users):
        place += mine[user : user + 1] * (start * UNIT + rank[user : user + 1])
        runs.append(units[user : user + 1])
        start += runs[-1]
    return place.astype(I32), runs


def sort_kernel(users, users_hbm, q_hbm, out_ref, users_ref, q_ref, sems):
    count, width = q_ref.shape
    rows = data_rows(count, users)
    fetch_users = pltpu.make_async_copy(users_hbm, users_ref, sems.at[0])
    fetch_q = pltpu.make_async_copy(q_hbm, q_ref, sems.at[1])
    fetch_users.start()
    fetch_q.start()
    fetch_users.wait()
    place, runs = placing(users_ref[...], users)
    onehot = jnp.where(lax.broadcasted_iota(I32, (rows, count), 0) == place, 1.0, 0.0).astype(BF16)
    lane = lax.broadcasted_iota(I32, (UNIT, width), 1)
    head = jnp.zeros((UNIT, width), F32)
    for user in range(users):
        head += jnp.where(lane == user, runs[user], 0.0)
    out_ref[rows:] = head.astype(BF16)
    fetch_q.wait()
    out_ref[:rows] = jnp.dot(onehot, q_ref[...], preferred_element_type=F32).astype(BF16)


def prepare_kernel(
    meta_ref, lengths_hbm, k_hbm, v_hbm, k_other, v_other, k_out, v_out, lengths_ref, k_own, v_own, sems
):
    users, chunk, width = k_own.shape
    fetches = [
        pltpu.make_async_copy(source, target, sems.at[i])
        for i, (source, target) in enumerate(((lengths_hbm, lengths_ref), (k_hbm, k_own), (v_hbm, v_own)))
    ]
    for fetch in fetches:
        fetch.start()
    for fetch in fetches:
        fetch.wait()
    rank = meta_ref[0]
    core = lax.rem(rank, 2)
    down = lax.broadcasted_iota(I32, (chunk, width), 0)
    along = lax.broadcasted_iota(I32, (width, chunk), 1)
    for user in range(users):
        first = jnp.where(core == 0, k_own[user, :UNIT].astype(F32), k_other[user, :UNIT].astype(F32))[:1]
        for k_ref, v_ref, slot, block in (
            (k_own, v_own, core, rank),
            (k_other, v_other, 1 - core, rank + 1 - 2 * core),
        ):
            usable = lengths_ref[user] - block * chunk
            at = pl.ds(pl.multiple_of(slot * chunk, chunk), chunk)
            k_out[user, at, :] = jnp.where(down < usable, k_ref[user].astype(F32), first).astype(BF16)
            turned = jnp.transpose(v_ref[user].astype(F32))
            v_out[user, :width, at] = jnp.where(along < usable, turned, 0.0).astype(BF16)
            v_out[user, width:, at] = jnp.where(along[:UNIT] < usable, 1.0, 0.0).astype(BF16)


def attend_scratch(blocks, rows, width, users=4, held=2048):
    most = attend_rows(blocks, rows, users)
    return [
        pltpu.VMEM((most, width), BF16),
        pltpu.VMEM((most, width), BF16),
        pltpu.VMEM((most, width), F32),
        pltpu.VMEM((held, TILE), F32),
        pltpu.VMEM((held, TILE), F32),
        pltpu.VMEM((width + 2 * UNIT, TILE), F32),
        pltpu.VMEM((16, width), I32),
        pltpu.SMEM((16, width), I32),
        pltpu.SMEM((2, 64), I32),
        pltpu.SemaphoreType.DMA,
    ]


def attend_rows(blocks, rows, users):
    return -(-(blocks * rows + users * (TILE - UNIT)) // TILE) * TILE + TILE + UNIT


def attend_kernel(users, blocks, meta_ref, lengths_ref, k_ref, v_ref, *refs):
    q_refs, out_refs = refs[:blocks], refs[blocks : 2 * blocks]
    sorted_q, pooled, stats, scores_a, scores_b, late, table, spots, tiles, sem = refs[2 * blocks :]
    width = k_ref.shape[2]
    held = k_ref.shape[1]
    rows = q_refs[0].shape[0] - UNIT
    score_scale = 1.0 / math.sqrt(width)
    factor = score_scale * math.log2(math.e)
    idle = attend_rows(blocks, rows, users) // UNIT - 1
    per_tile = TILE // UNIT

    heads = jnp.concatenate(
        [ref[rows:].astype(F32)[:1] for ref in q_refs] + [jnp.zeros((1, width), F32)] * (8 - blocks), axis=0
    )
    sub = lax.broadcasted_iota(I32, (8, width), 0)
    lane = lax.broadcasted_iota(I32, (8, width), 1)
    unit = lane.astype(F32)
    ahead = jnp.zeros((8, width), F32)
    for block in range(blocks):
        ahead += jnp.where(sub > block, heads[block : block + 1], 0.0)
    totals = jnp.sum(heads, axis=0, keepdims=True)
    begin = jnp.zeros((1, 1), F32)
    within = jnp.zeros((8, 1), F32)
    spot = unit
    facts = jnp.zeros((8, width), F32)
    for user in range(users):
        spot = jnp.where(unit >= within, unit - within + begin + ahead[:, user : user + 1], spot)
        within += heads[:, user : user + 1]
        count = jnp.floor((totals[:, user : user + 1] + (per_tile - 1)) * (1.0 / per_tile))
        facts = jnp.where(lane == user, begin, jnp.where(lane == 8 + user, count, facts))
        begin += count * per_tile
    spot = jnp.where(unit >= within, float(idle), spot)
    table[:8] = spot.astype(I32)
    table[8:] = facts.astype(I32)
    copy = pltpu.make_async_copy(table, spots, sem)
    copy.start()
    copy.wait()

    def spot_of(block, unit):
        return pl.ds(pl.multiple_of(spots[block, unit] * UNIT, UNIT), UNIT)

    units = rows // UNIT
    for block in range(blocks):
        for unit in range(units):
            sorted_q[spot_of(block, unit), :] = q_refs[block][unit * UNIT : (unit + 1) * UNIT]
    pooled[idle * UNIT :] = jnp.zeros((UNIT, width), BF16)
    stats[idle * UNIT :] = jnp.zeros((UNIT, width), F32)

    def tile_at(row):
        return pl.ds(pl.multiple_of(row, TILE), TILE)

    part = lax.rem(lax.broadcasted_iota(I32, (width, TILE), 0), 16) // 5

    def finish(row, sums, largest):
        total = sums[width : width + 1]
        level = largest * score_scale + jnp.log(total)
        high = level.astype(BF16).astype(F32)
        rest = level - high
        middle = rest.astype(BF16).astype(F32)
        pooled[tile_at(row), :] = jnp.transpose(sums[:width] * (1.0 / total)).astype(BF16)
        stats[tile_at(row), :] = jnp.transpose(
            jnp.where(part == 0, high, jnp.where(part == 1, middle, rest - middle))
        )

    def score(buffer, user, query, best, j):
        scores = lax.dot_general(
            k_ref[user, j * STRIP : (j + 1) * STRIP],
            query,
            (((1,), (1,)), ((), ())),
            preferred_element_type=F32,
        )
        buffer[j * STRIP : (j + 1) * STRIP, :] = scores
        strip = jnp.max(scores.reshape(STRIP // 8, 8, TILE), axis=0)
        return strip if best is None else jnp.maximum(best, strip)

    def weigh(buffer, user, scaled, sums, j):
        weights = jnp.exp2(buffer[j * STRIP : (j + 1) * STRIP, :] * factor - scaled).astype(BF16)
        more = jnp.dot(v_ref[user, :, j * STRIP : (j + 1) * STRIP], weights, preferred_element_type=F32)
        return more if sums is None else sums + more

    def both(ahead, ahead_buffer, now, now_buffer, best, done_row, done_sums, done_largest):
        user, row = tiles[0, ahead], tiles[1, ahead]
        now_user, now_row = tiles[0, now], tiles[1, now]
        query = sorted_q[tile_at(row), :]
        largest = jnp.max(best, axis=0, keepdims=True)
        scaled = largest * factor
        best, sums = None, None
        for j in range(held // STRIP):
            best = score(ahead_buffer, user, query, best, j)
            sums = weigh(now_buffer, now_user, scaled, sums, j)
            if j == 1:
                finish(done_row, done_sums, done_largest)
        return best, now_row, sums, largest

    def few_step(user, count, i, carry):
        rows = [spots[8, user] * UNIT + jnp.minimum(3 * i + t, count - 1) * TILE for t in range(3)]
        scores = [
            lax.dot_general(
                k_ref[user, :STRIP],
                sorted_q[tile_at(row), :],
                (((1,), (1,)), ((), ())),
                preferred_element_type=F32,
            )
            for row in rows
        ]
        largest = [jnp.max(score, axis=0, keepdims=True) for score in scores]
        weights = [jnp.exp2(score * factor - top * factor).astype(BF16) for score, top in zip(scores, largest)]
        sums = [jnp.dot(v_ref[user, :, :STRIP], weight, preferred_element_type=F32) for weight in weights]
        for row, total, top in zip(rows, sums, largest):
            finish(row, total, top)
        return carry

    def skip_step(user, i, carry):
        row = spots[8, user] * UNIT + i * TILE
        empty = jnp.full((1, TILE), EMPTY, F32)
        sums = jnp.where(lax.broadcasted_iota(I32, (width + UNIT, TILE), 0) < width, 0.0, 1.0)
        finish(row, sums, empty * (1.0 / score_scale))
        return carry

    full = jnp.int32(0)
    for user in range(users):
        usable = lengths_ref[user] - (meta_ref[0] // 2) * held
        count = spots[8, 8 + user]
        many = usable > STRIP

        def enter(i, carry, user=user, full=full):
            tiles[0, full + i] = jnp.int32(user)
            tiles[1, full + i] = spots[8, user] * UNIT + i * TILE
            return carry

        listed = jnp.where(many, count, 0)
        lax.fori_loop(0, listed, enter, 0)
        full = full + listed
        lax.fori_loop(
            0,
            jnp.where((usable > 0) & (usable <= STRIP), (count + 2) // 3, 0),
            functools.partial(few_step, user, count),
            0,
        )
        lax.fori_loop(0, jnp.where(usable <= 0, count, 0), functools.partial(skip_step, user), 0)

    @pl.when(full > 0)
    def _():
        query = sorted_q[tile_at(tiles[1, 0]), :]
        best = None
        for j in range(held // STRIP):
            best = score(scores_a, tiles[0, 0], query, best, j)

        def kept():
            return late[: width + UNIT], late[width + UNIT : width + UNIT + 1]

        def pair(i, carry):
            best, row = carry
            last = full - 1
            second = jnp.minimum(2 * i + 1, last)
            best, *done = both(second, scores_b, 2 * i, scores_a, best, row, *kept())
            best, row, sums, largest = both(
                jnp.minimum(2 * i + 2, last), scores_a, second, scores_b, best, *done
            )
            late[: width + UNIT] = sums
            late[width + UNIT :] = jnp.broadcast_to(largest, (UNIT, TILE))
            return best, row

        _, row = lax.fori_loop(0, (full + 1) // 2, pair, (best, jnp.int32(idle * UNIT - TILE)))
        finish(row, *kept())

    lane = lax.broadcasted_iota(I32, (UNIT, width), 1)
    code = jnp.where(lax.rem(lane, 16) == 15, -1, (lane // 16) * 8 + lax.rem(lax.rem(lane, 16), 5))
    turned = []
    for place in range(8):
        held_rows = jnp.zeros((UNIT, width), F32)
        for unit in range(place, units, 8):
            for block in range(blocks):
                held_rows = jnp.where(code == block * 8 + unit // 8, stats[spot_of(block, unit), :], held_rows)
        turned.append(held_rows)
    levels = jnp.transpose(jnp.concatenate(turned, axis=0)).astype(BF16)
    for block in range(blocks):
        for unit in range(units):
            out_refs[block][unit * UNIT : (unit + 1) * UNIT] = pooled[spot_of(block, unit), :]
        out_refs[block][rows:] = levels[block * 16 : block * 16 + 16]


GROUPS = 5


def levels_of(ref, rows):
    pieces = ref[rows:].astype(F32)
    return pieces[0:5] + pieces[5:10] + pieces[10:15]


def blend(levels, refs, rows):
    width = refs[0].shape[1]
    largest = functools.reduce(jnp.maximum, levels)
    shares = [jnp.exp(level - largest) for level in levels]
    whole = sum(shares)
    gap = jnp.zeros((8 - GROUPS, width), F32)
    stacked = jnp.concatenate([x for share in shares for x in (share / whole, gap)], axis=0)
    stacked = jnp.concatenate([stacked, jnp.zeros((128 - stacked.shape[0], width), F32)], axis=0)
    columns = jnp.transpose(stacked)
    means = []
    for group in range(GROUPS):
        size = min(128, rows - group * 128)
        total = jnp.zeros((size, width), F32)
        for i, ref in enumerate(refs):
            share = columns[:size, i * 8 + group : i * 8 + group + 1]
            total += share * ref[group * 128 : group * 128 + size].astype(F32)
        means.append(total)
    return means, largest + jnp.log(whole)


def gather_kernel(users, users_ref, *refs):
    part_refs, (onehot_ref, mean_ref, level_ref) = refs[:-3], refs[-3:]
    rows = mean_ref.shape[0]
    count = users_ref.shape[1]
    means, level = blend([levels_of(ref, rows) for ref in part_refs], part_refs, rows)
    for group, mean in enumerate(means):
        mean_ref[group * 128 : group * 128 + mean.shape[0]] = mean
    level_ref[...] = jnp.concatenate([level, jnp.zeros((8 - GROUPS, level.shape[1]), F32)], axis=0)
    place, _ = placing(users_ref[...], users)
    onehot_ref[...] = jnp.where(lax.broadcasted_iota(I32, (rows, count), 0) == place, 1.0, 0.0).astype(BF16)


def merge_kernel(onehot_ref, mean_ref, level_ref, *refs):
    part_refs, out_ref = refs[:-1], refs[-1]
    rows = mean_ref.shape[0]
    levels = [level_ref[:GROUPS]] + [levels_of(ref, rows) for ref in part_refs]
    means, _ = blend(levels, [mean_ref, *part_refs], rows)
    merged = jnp.concatenate([mean.astype(BF16) for mean in means], axis=0)
    out_ref[...] = lax.dot_general(
        onehot_ref[...], merged, (((0,), (0,)), ((), ())), preferred_element_type=F32
    ).astype(BF16)


def local(layout, queries, users_of, keys, values, lengths):
    count, width = queries.shape
    users, chunk, _ = keys.shape
    rows = data_rows(count, users)
    zs, xs = layout

    def shift(dz, dx, dc):
        def place(z, x, c):
            return (z * xs + x) * 2 + c

        return [
            (place(z, x, c), place((z + dz) % zs, (x + dx) % xs, c ^ dc))
            for z in range(zs)
            for x in range(xs)
            for c in range(2)
        ]

    near = [(0, 2), (1, 2)]
    far = [(1, 1), (1, 3), (0, 1), (0, 3), (1, 0)]
    meta = lax.axis_index("seq").astype(I32).reshape(1)
    users_row = users_of.reshape(1, count)
    message = jax.ShapeDtypeStruct((rows + UNIT, width), BF16)

    sent = pl.pallas_call(
        functools.partial(sort_kernel, users),
        out_shape=message,
        in_specs=[HBM, HBM],
        out_specs=VMEM,
        scratch_shapes=[
            pltpu.VMEM((1, count), I32),
            pltpu.VMEM((count, width), BF16),
            pltpu.SemaphoreType.DMA((2,)),
        ],
        compiler_params=params(8),
        cost_estimate=pl.CostEstimate(flops=2*10**9, bytes_accessed=10**6, transcendentals=0),
    )(users_row, queries)
    k_other = lax.ppermute(keys, "seq", shift(0, 0, 1))
    v_other = lax.ppermute(values, "seq", shift(0, 0, 1))
    far_in = [lax.ppermute(sent, "seq", shift(dz, dx, 0)) for dz, dx in far]
    near_in = [lax.ppermute(sent, "seq", shift(dz, dx, 0)) for dz, dx in near]

    k_held, v_held = pl.pallas_call(
        prepare_kernel,
        out_shape=(
            jax.ShapeDtypeStruct((users, 2 * chunk, width), BF16),
            jax.ShapeDtypeStruct((users, width + UNIT, 2 * chunk), BF16),
        ),
        in_specs=[SMEM, HBM, HBM, HBM, VMEM, VMEM],
        out_specs=(VMEM, VMEM),
        scratch_shapes=[
            pltpu.SMEM((users,), I32),
            pltpu.VMEM(keys.shape, BF16),
            pltpu.VMEM(values.shape, BF16),
            pltpu.SemaphoreType.DMA((3,)),
        ],
        compiler_params=params(20),
        cost_estimate=pl.CostEstimate(flops=10**8, bytes_accessed=10**7, transcendentals=0),
    )(meta, lengths, keys, values, k_other, v_other)

    def attend(arrived):
        blocks = len(arrived)
        return pl.pallas_call(
            functools.partial(attend_kernel, users, blocks),
            out_shape=[message] * blocks,
            in_specs=[SMEM, SMEM] + [VMEM] * (2 + blocks),
            out_specs=[VMEM] * blocks,
            scratch_shapes=attend_scratch(blocks, rows, width, users, 2 * chunk),
            compiler_params=params(24),
            cost_estimate=pl.CostEstimate(flops=10**10, bytes_accessed=10**7, transcendentals=0),
        )(meta, lengths, k_held, v_held, *arrived)

    far_out = attend(far_in)
    far_back = [lax.ppermute(part, "seq", shift(-dz, -dx, 0)) for part, (dz, dx) in zip(far_out, far)]
    own, *near_out = attend([sent, *near_in])
    near_back = [lax.ppermute(part, "seq", shift(-dz, -dx, 0)) for part, (dz, dx) in zip(near_out, near)]

    onehot, mean, level = pl.pallas_call(
        functools.partial(gather_kernel, users),
        out_shape=(
            jax.ShapeDtypeStruct((rows, count), BF16),
            jax.ShapeDtypeStruct((rows, width), F32),
            jax.ShapeDtypeStruct((8, width), F32),
        ),
        in_specs=[VMEM] * (1 + len(far)),
        out_specs=(VMEM, VMEM, VMEM),
        compiler_params=params(8),
        cost_estimate=pl.CostEstimate(flops=10**9, bytes_accessed=10**6, transcendentals=0),
    )(users_row, *far_back)
    return pl.pallas_call(
        merge_kernel,
        out_shape=jax.ShapeDtypeStruct((count, width), BF16),
        in_specs=[VMEM] * (4 + len(near)),
        out_specs=VMEM,
        compiler_params=params(8),
    )(onehot, mean, level, own, *near_back)


def solution(mesh):
    seq = mesh.shape["seq"]
    layout = (2, seq // 4)
    return jax.shard_map(
        functools.partial(local, layout),
        mesh=mesh,
        in_specs=(
            P(("dp", "seq"), None),
            P(("dp", "seq")),
            P("dp", "seq", None),
            P("dp", "seq", None),
            P("dp"),
        ),
        out_specs=P(("dp", "seq"), None),
        check_vma=False,
    )
```

```python
import functools
import math

import jax
import jax.numpy as jnp
from jax import lax
from jax.experimental import pallas as pl
from jax.experimental.pallas import tpu as pltpu
from jax.sharding import PartitionSpec as P


F32 = jnp.float32
BF16 = jnp.bfloat16
I32 = jnp.int32
UNIT = 16
TILE = 256
STRIP = 256
EMPTY = -1e30
VMEM = pl.BlockSpec(memory_space=pltpu.VMEM)
SMEM = pl.BlockSpec(memory_space=pltpu.SMEM)
HBM = pl.BlockSpec(memory_space=pltpu.HBM)


def params(mebibytes):
    return pltpu.CompilerParams(vmem_limit_bytes=mebibytes * 1024 * 1024)


def data_rows(count, users):
    return count + (users - 1) * UNIT


def placing(users_row, users):
    count = users_row.shape[1]
    ids = lax.broadcasted_iota(I32, (8, count), 0)
    mine = jnp.where(ids == users_row, 1.0, 0.0).astype(F32)
    before = jnp.where(
        lax.broadcasted_iota(I32, (count, count), 0) < lax.broadcasted_iota(I32, (count, count), 1), 1.0, 0.0
    ).astype(BF16)
    rank = jnp.dot(mine.astype(BF16), before, preferred_element_type=F32)
    units = jnp.floor((jnp.sum(mine, axis=1, keepdims=True) + (UNIT - 1)) * (1.0 / UNIT))
    start = jnp.zeros((1, 1), F32)
    place = jnp.zeros((1, count), F32)
    runs = []
    for user in range(users):
        place += mine[user : user + 1] * (start * UNIT + rank[user : user + 1])
        runs.append(units[user : user + 1])
        start += runs[-1]
    return place.astype(I32), runs


def sort_kernel(users, users_hbm, q_hbm, out_ref, users_ref, q_ref, sems):
    count, width = q_ref.shape
    rows = data_rows(count, users)
    fetch_users = pltpu.make_async_copy(users_hbm, users_ref, sems.at[0])
    fetch_q = pltpu.make_async_copy(q_hbm, q_ref, sems.at[1])
    fetch_users.start()
    fetch_q.start()
    fetch_users.wait()
    place, runs = placing(users_ref[...], users)
    onehot = jnp.where(lax.broadcasted_iota(I32, (rows, count), 0) == place, 1.0, 0.0).astype(BF16)
    lane = lax.broadcasted_iota(I32, (UNIT, width), 1)
    head = jnp.zeros((UNIT, width), F32)
    for user in range(users):
        head += jnp.where(lane == user, runs[user], 0.0)
    out_ref[rows:] = head.astype(BF16)
    fetch_q.wait()
    out_ref[:rows] = jnp.dot(onehot, q_ref[...], preferred_element_type=F32).astype(BF16)


def prepare_kernel(
    meta_ref, lengths_hbm, k_hbm, v_hbm, k_other, v_other, k_out, v_out, lengths_ref, k_own, v_own, sems
):
    users, chunk, width = k_own.shape
    fetches = [
        pltpu.make_async_copy(source, target, sems.at[i])
        for i, (source, target) in enumerate(((lengths_hbm, lengths_ref), (k_hbm, k_own), (v_hbm, v_own)))
    ]
    for fetch in fetches:
        fetch.start()
    for fetch in fetches:
        fetch.wait()
    rank = meta_ref[0]
    core = lax.rem(rank, 2)
    down = lax.broadcasted_iota(I32, (chunk, width), 0)
    along = lax.broadcasted_iota(I32, (width, chunk), 1)
    for user in range(users):
        first = jnp.where(core == 0, k_own[user, :UNIT].astype(F32), k_other[user, :UNIT].astype(F32))[:1]
        for k_ref, v_ref, slot, block in (
            (k_own, v_own, core, rank),
            (k_other, v_other, 1 - core, rank + 1 - 2 * core),
        ):
            usable = lengths_ref[user] - block * chunk
            at = pl.ds(pl.multiple_of(slot * chunk, chunk), chunk)
            k_out[user, at, :] = jnp.where(down < usable, k_ref[user].astype(F32), first).astype(BF16)
            turned = jnp.transpose(v_ref[user].astype(F32))
            v_out[user, :width, at] = jnp.where(along < usable, turned, 0.0).astype(BF16)
            v_out[user, width:, at] = jnp.where(along[:UNIT] < usable, 1.0, 0.0).astype(BF16)


def attend_scratch(blocks, rows, width, users=4, held=2048):
    most = attend_rows(blocks, rows, users)
    return [
        pltpu.VMEM((most, width), BF16),
        pltpu.VMEM((most, width), BF16),
        pltpu.VMEM((most, width), F32),
        pltpu.VMEM((held, TILE), F32),
        pltpu.VMEM((held, TILE), F32),
        pltpu.VMEM((width + 2 * UNIT, TILE), F32),
        pltpu.VMEM((16, width), I32),
        pltpu.SMEM((16, width), I32),
        pltpu.SMEM((2, 64), I32),
        pltpu.SemaphoreType.DMA,
    ]


def attend_rows(blocks, rows, users):
    return -(-(blocks * rows + users * (TILE - UNIT)) // TILE) * TILE + TILE + UNIT


def attend_kernel(users, blocks, meta_ref, lengths_ref, k_ref, v_ref, *refs):
    q_refs, out_refs = refs[:blocks], refs[blocks : 2 * blocks]
    sorted_q, pooled, stats, scores_a, scores_b, late, table, spots, tiles, sem = refs[2 * blocks :]
    width = k_ref.shape[2]
    held = k_ref.shape[1]
    rows = q_refs[0].shape[0] - UNIT
    score_scale = 1.0 / math.sqrt(width)
    factor = score_scale * math.log2(math.e)
    idle = attend_rows(blocks, rows, users) // UNIT - 1
    per_tile = TILE // UNIT

    heads = jnp.concatenate(
        [ref[rows:].astype(F32)[:1] for ref in q_refs] + [jnp.zeros((1, width), F32)] * (8 - blocks), axis=0
    )
    sub = lax.broadcasted_iota(I32, (8, width), 0)
    lane = lax.broadcasted_iota(I32, (8, width), 1)
    unit = lane.astype(F32)
    ahead = jnp.zeros((8, width), F32)
    for block in range(blocks):
        ahead += jnp.where(sub > block, heads[block : block + 1], 0.0)
    totals = jnp.sum(heads, axis=0, keepdims=True)
    begin = jnp.zeros((1, 1), F32)
    within = jnp.zeros((8, 1), F32)
    spot = unit
    facts = jnp.zeros((8, width), F32)
    for user in range(users):
        spot = jnp.where(unit >= within, unit - within + begin + ahead[:, user : user + 1], spot)
        within += heads[:, user : user + 1]
        count = jnp.floor((totals[:, user : user + 1] + (per_tile - 1)) * (1.0 / per_tile))
        facts = jnp.where(lane == user, begin, jnp.where(lane == 8 + user, count, facts))
        begin += count * per_tile
    spot = jnp.where(unit >= within, float(idle), spot)
    table[:8] = spot.astype(I32)
    table[8:] = facts.astype(I32)
    copy = pltpu.make_async_copy(table, spots, sem)
    copy.start()
    copy.wait()

    def spot_of(block, unit):
        return pl.ds(pl.multiple_of(spots[block, unit] * UNIT, UNIT), UNIT)

    units = rows // UNIT
    for block in range(blocks):
        for unit in range(units):
            sorted_q[spot_of(block, unit), :] = q_refs[block][unit * UNIT : (unit + 1) * UNIT]
    pooled[idle * UNIT :] = jnp.zeros((UNIT, width), BF16)
    stats[idle * UNIT :] = jnp.zeros((UNIT, width), F32)

    def tile_at(row):
        return pl.ds(pl.multiple_of(row, TILE), TILE)

    part = lax.rem(lax.broadcasted_iota(I32, (width, TILE), 0), 16) // 5

    def finish(row, sums, largest):
        total = sums[width : width + 1]
        level = largest * score_scale + jnp.log(total)
        high = level.astype(BF16).astype(F32)
        rest = level - high
        middle = rest.astype(BF16).astype(F32)
        pooled[tile_at(row), :] = jnp.transpose(sums[:width] * (1.0 / total)).astype(BF16)
        stats[tile_at(row), :] = jnp.transpose(
            jnp.where(part == 0, high, jnp.where(part == 1, middle, rest - middle))
        )

    def score(buffer, user, query, best, j):
        scores = lax.dot_general(
            k_ref[user, j * STRIP : (j + 1) * STRIP],
            query,
            (((1,), (1,)), ((), ())),
            preferred_element_type=F32,
        )
        buffer[j * STRIP : (j + 1) * STRIP, :] = scores
        strip = jnp.max(scores.reshape(STRIP // 8, 8, TILE), axis=0)
        return strip if best is None else jnp.maximum(best, strip)

    def weigh(buffer, user, scaled, sums, j):
        weights = jnp.exp2(buffer[j * STRIP : (j + 1) * STRIP, :] * factor - scaled).astype(BF16)
        more = jnp.dot(v_ref[user, :, j * STRIP : (j + 1) * STRIP], weights, preferred_element_type=F32)
        return more if sums is None else sums + more

    def both(ahead, ahead_buffer, now, now_buffer, best, done_row, done_sums, done_largest):
        user, row = tiles[0, ahead], tiles[1, ahead]
        now_user, now_row = tiles[0, now], tiles[1, now]
        query = sorted_q[tile_at(row), :]
        largest = jnp.max(best, axis=0, keepdims=True)
        scaled = largest * factor
        best, sums = None, None
        for j in range(held // STRIP):
            best = score(ahead_buffer, user, query, best, j)
            sums = weigh(now_buffer, now_user, scaled, sums, j)
            if j == 1:
                finish(done_row, done_sums, done_largest)
        return best, now_row, sums, largest

    def few_step(user, count, i, carry):
        rows = [spots[8, user] * UNIT + jnp.minimum(3 * i + t, count - 1) * TILE for t in range(3)]
        scores = [
            lax.dot_general(
                k_ref[user, :STRIP],
                sorted_q[tile_at(row), :],
                (((1,), (1,)), ((), ())),
                preferred_element_type=F32,
            )
            for row in rows
        ]
        largest = [jnp.max(score, axis=0, keepdims=True) for score in scores]
        weights = [jnp.exp2(score * factor - top * factor).astype(BF16) for score, top in zip(scores, largest)]
        sums = [jnp.dot(v_ref[user, :, :STRIP], weight, preferred_element_type=F32) for weight in weights]
        for row, total, top in zip(rows, sums, largest):
            finish(row, total, top)
        return carry

    def skip_step(user, i, carry):
        row = spots[8, user] * UNIT + i * TILE
        empty = jnp.full((1, TILE), EMPTY, F32)
        sums = jnp.where(lax.broadcasted_iota(I32, (width + UNIT, TILE), 0) < width, 0.0, 1.0)
        finish(row, sums, empty * (1.0 / score_scale))
        return carry

    full = jnp.int32(0)
    for user in range(users):
        usable = lengths_ref[user] - (meta_ref[0] // 2) * held
        count = spots[8, 8 + user]
        many = usable > STRIP

        def enter(i, carry, user=user, full=full):
            tiles[0, full + i] = jnp.int32(user)
            tiles[1, full + i] = spots[8, user] * UNIT + i * TILE
            return carry

        listed = jnp.where(many, count, 0)
        lax.fori_loop(0, listed, enter, 0)
        full = full + listed
        lax.fori_loop(
            0,
            jnp.where((usable > 0) & (usable <= STRIP), (count + 2) // 3, 0),
            functools.partial(few_step, user, count),
            0,
        )
        lax.fori_loop(0, jnp.where(usable <= 0, count, 0), functools.partial(skip_step, user), 0)

    @pl.when(full > 0)
    def _():
        query = sorted_q[tile_at(tiles[1, 0]), :]
        best = None
        for j in range(held // STRIP):
            best = score(scores_a, tiles[0, 0], query, best, j)

        def kept():
            return late[: width + UNIT], late[width + UNIT : width + UNIT + 1]

        def pair(i, carry):
            best, row = carry
            last = full - 1
            second = jnp.minimum(2 * i + 1, last)
            best, *done = both(second, scores_b, 2 * i, scores_a, best, row, *kept())
            best, row, sums, largest = both(
                jnp.minimum(2 * i + 2, last), scores_a, second, scores_b, best, *done
            )
            late[: width + UNIT] = sums
            late[width + UNIT :] = jnp.broadcast_to(largest, (UNIT, TILE))
            return best, row

        _, row = lax.fori_loop(0, (full + 1) // 2, pair, (best, jnp.int32(idle * UNIT - TILE)))
        finish(row, *kept())

    lane = lax.broadcasted_iota(I32, (UNIT, width), 1)
    code = jnp.where(lax.rem(lane, 16) == 15, -1, (lane // 16) * 8 + lax.rem(lax.rem(lane, 16), 5))
    turned = []
    for place in range(8):
        held_rows = jnp.zeros((UNIT, width), F32)
        for unit in range(place, units, 8):
            for block in range(blocks):
                held_rows = jnp.where(code == block * 8 + unit // 8, stats[spot_of(block, unit), :], held_rows)
        turned.append(held_rows)
    levels = jnp.transpose(jnp.concatenate(turned, axis=0)).astype(BF16)
    for block in range(blocks):
        for unit in range(units):
            out_refs[block][unit * UNIT : (unit + 1) * UNIT] = pooled[spot_of(block, unit), :]
        out_refs[block][rows:] = levels[block * 16 : block * 16 + 16]


GROUPS = 5


def levels_of(ref, rows):
    pieces = ref[rows:].astype(F32)
    return pieces[0:5] + pieces[5:10] + pieces[10:15]


def blend(levels, refs, rows):
    width = refs[0].shape[1]
    largest = functools.reduce(jnp.maximum, levels)
    shares = [jnp.exp(level - largest) for level in levels]
    whole = sum(shares)
    gap = jnp.zeros((8 - GROUPS, width), F32)
    stacked = jnp.concatenate([x for share in shares for x in (share / whole, gap)], axis=0)
    stacked = jnp.concatenate([stacked, jnp.zeros((128 - stacked.shape[0], width), F32)], axis=0)
    columns = jnp.transpose(stacked)
    means = []
    for group in range(GROUPS):
        size = min(128, rows - group * 128)
        total = jnp.zeros((size, width), F32)
        for i, ref in enumerate(refs):
            share = columns[:size, i * 8 + group : i * 8 + group + 1]
            total += share * ref[group * 128 : group * 128 + size].astype(F32)
        means.append(total)
    return means, largest + jnp.log(whole)


def gather_kernel(users, users_ref, *refs):
    part_refs, (onehot_ref, mean_ref, level_ref) = refs[:-3], refs[-3:]
    rows = mean_ref.shape[0]
    count = users_ref.shape[1]
    means, level = blend([levels_of(ref, rows) for ref in part_refs], part_refs, rows)
    for group, mean in enumerate(means):
        mean_ref[group * 128 : group * 128 + mean.shape[0]] = mean
    level_ref[...] = jnp.concatenate([level, jnp.zeros((8 - GROUPS, level.shape[1]), F32)], axis=0)
    place, _ = placing(users_ref[...], users)
    onehot_ref[...] = jnp.where(lax.broadcasted_iota(I32, (rows, count), 0) == place, 1.0, 0.0).astype(BF16)


def merge_kernel(onehot_ref, mean_ref, level_ref, *refs):
    part_refs, out_ref = refs[:-1], refs[-1]
    rows = mean_ref.shape[0]
    levels = [level_ref[:GROUPS]] + [levels_of(ref, rows) for ref in part_refs]
    means, _ = blend(levels, [mean_ref, *part_refs], rows)
    merged = jnp.concatenate([mean.astype(BF16) for mean in means], axis=0)
    out_ref[...] = lax.dot_general(
        onehot_ref[...], merged, (((0,), (0,)), ((), ())), preferred_element_type=F32
    ).astype(BF16)


def local(layout, queries, users_of, keys, values, lengths):
    count, width = queries.shape
    users, chunk, _ = keys.shape
    rows = data_rows(count, users)
    zs, xs = layout

    def shift(dz, dx, dc):
        def place(z, x, c):
            return (z * xs + x) * 2 + c

        return [
            (place(z, x, c), place((z + dz) % zs, (x + dx) % xs, c ^ dc))
            for z in range(zs)
            for x in range(xs)
            for c in range(2)
        ]

    near = [(0, 2), (1, 2)]
    far = [(1, 1), (1, 3), (0, 1), (0, 3), (1, 0)]
    meta = lax.axis_index("seq").astype(I32).reshape(1)
    users_row = users_of.reshape(1, count)
    message = jax.ShapeDtypeStruct((rows + UNIT, width), BF16)

    sent = pl.pallas_call(
        functools.partial(sort_kernel, users),
        out_shape=message,
        in_specs=[HBM, HBM],
        out_specs=VMEM,
        scratch_shapes=[
            pltpu.VMEM((1, count), I32),
            pltpu.VMEM((count, width), BF16),
            pltpu.SemaphoreType.DMA((2,)),
        ],
        compiler_params=params(60),
        cost_estimate=pl.CostEstimate(flops=2*10**9, bytes_accessed=10**6, transcendentals=0),
    )(users_row, queries)
    k_other = lax.ppermute(keys, "seq", shift(0, 0, 1))
    v_other = lax.ppermute(values, "seq", shift(0, 0, 1))
    far_in = [lax.ppermute(sent, "seq", shift(dz, dx, 0)) for dz, dx in far]
    near_in = [lax.ppermute(sent, "seq", shift(dz, dx, 0)) for dz, dx in near]

    k_held, v_held = pl.pallas_call(
        prepare_kernel,
        out_shape=(
            jax.ShapeDtypeStruct((users, 2 * chunk, width), BF16),
            jax.ShapeDtypeStruct((users, width + UNIT, 2 * chunk), BF16),
        ),
        in_specs=[SMEM, HBM, HBM, HBM, VMEM, VMEM],
        out_specs=(VMEM, VMEM),
        scratch_shapes=[
            pltpu.SMEM((users,), I32),
            pltpu.VMEM(keys.shape, BF16),
            pltpu.VMEM(values.shape, BF16),
            pltpu.SemaphoreType.DMA((3,)),
        ],
        compiler_params=params(20),
        cost_estimate=pl.CostEstimate(flops=10**8, bytes_accessed=10**7, transcendentals=0),
    )(meta, lengths, keys, values, k_other, v_other)

    def attend(arrived):
        blocks = len(arrived)
        return pl.pallas_call(
            functools.partial(attend_kernel, users, blocks),
            out_shape=[message] * blocks,
            in_specs=[SMEM, SMEM] + [VMEM] * (2 + blocks),
            out_specs=[VMEM] * blocks,
            scratch_shapes=attend_scratch(blocks, rows, width, users, 2 * chunk),
            compiler_params=params(24),
            cost_estimate=pl.CostEstimate(flops=10**10, bytes_accessed=10**7, transcendentals=0),
        )(meta, lengths, k_held, v_held, *arrived)

    far_out = attend(far_in)
    far_back = [lax.ppermute(part, "seq", shift(-dz, -dx, 0)) for part, (dz, dx) in zip(far_out, far)]
    own, *near_out = attend([sent, *near_in])
    near_back = [lax.ppermute(part, "seq", shift(-dz, -dx, 0)) for part, (dz, dx) in zip(near_out, near)]

    onehot, mean, level = pl.pallas_call(
        functools.partial(gather_kernel, users),
        out_shape=(
            jax.ShapeDtypeStruct((rows, count), BF16),
            jax.ShapeDtypeStruct((rows, width), F32),
            jax.ShapeDtypeStruct((8, width), F32),
        ),
        in_specs=[VMEM] * (1 + len(far)),
        out_specs=(VMEM, VMEM, VMEM),
        compiler_params=params(8),
        cost_estimate=pl.CostEstimate(flops=10**9, bytes_accessed=10**6, transcendentals=0),
    )(users_row, *far_back)
    return pl.pallas_call(
        merge_kernel,
        out_shape=jax.ShapeDtypeStruct((count, width), BF16),
        in_specs=[VMEM] * (4 + len(near)),
        out_specs=VMEM,
        compiler_params=params(8),
    )(onehot, mean, level, own, *near_back)


def solution(mesh):
    seq = mesh.shape["seq"]
    layout = (2, seq // 4)
    return jax.shard_map(
        functools.partial(local, layout),
        mesh=mesh,
        in_specs=(
            P(("dp", "seq"), None),
            P(("dp", "seq")),
            P("dp", "seq", None),
            P("dp", "seq", None),
            P("dp"),
        ),
        out_specs=P(("dp", "seq"), None),
        check_vma=False,
    )
```
